32 devices in a mesh: vp: 32 (over z, y, x, core).
Axes of the slice: x: 2, y: 2, z: 4, core: 2. Of those that a mesh axis runs over, the one named last changes fastest.
Arguments:
- residual: bfloat16 [8192, 1024], replicated
- labels: int32 [8192], replicated
- loss_mask: float32 [8192], replicated
- norm_gain: float32 [1024], replicated
- embed_table: bfloat16 [49408, 1024], P('vp')
Outputs:
- output 1: float32 [], replicated
- output 2: float32 [8192, 1024], P('vp')
- output 3: float32 [49408, 1024], P('vp')
- output 4: float32 [1024], replicated
All inputs are finite; a program needn't handle non-finite values.
Results may differ from the reference program's by a relative error of at most 0.001.
Values sent between devices are 32-bit elements.
A program may use at most 1 GiB of HBM per device.

```python
import jax
import jax.numpy as jnp
from jax import lax

TOKENS = 8192
DIM = 1024
VOCAB_REAL = 49155
VOCAB_PAD = 49408

LOGIT_SCALE = 6.0
NORM_EPS = 1e-6


def draw_labels(label_key):
    k_pick, k_wide, k_low = jax.random.split(label_key, 3)
    pick_wide = jax.random.randint(k_pick, (TOKENS,), 0, 2)
    wide_ids = jax.random.randint(k_wide, (TOKENS,), 0, VOCAB_REAL)
    low_ids = jax.random.randint(k_low, (TOKENS,), 0, VOCAB_REAL // 16)
    label_ids = jnp.where(pick_wide == 0, wide_ids, low_ids).astype(jnp.int32)
    return label_ids.at[0].set(0).at[1].set(VOCAB_REAL - 1)


def draw_mask(mask_key):
    keep_draw = jax.random.randint(mask_key, (TOKENS,), 0, 5)
    mask_vals = (keep_draw > 0).astype(jnp.float32)
    return mask_vals.at[0].set(1.0)


def setup_inputs(seed: int = 0) -> dict:
    base_key = jax.random.key(seed)
    k_table, k_noise, k_peak, k_gain, k_label, k_mask = jax.random.split(base_key, 6)
    emb_std = LOGIT_SCALE * DIM ** -0.5
    table_f32 = jax.random.normal(k_table, (VOCAB_PAD, DIM), jnp.float32) * emb_std
    peak_ids = jax.random.randint(k_peak, (TOKENS, 4), 0, VOCAB_REAL)
    peak_sum = jnp.zeros((TOKENS, DIM), jnp.float32)
    for peak in range(4):
        peak_sum = peak_sum + table_f32[peak_ids[:, peak]] / emb_std
    peak_weight = 14.0 * DIM ** -0.5
    noise = jax.random.normal(k_noise, (TOKENS, DIM), jnp.float32)
    residual = (noise + peak_weight * peak_sum).astype(jnp.bfloat16)
    norm_gain = 1.0 + 0.3 * jax.random.normal(k_gain, (DIM,), jnp.float32)
    return {
        'residual': residual,
        'labels': draw_labels(k_label),
        'loss_mask': draw_mask(k_mask),
        'norm_gain': norm_gain,
        'embed_table': table_f32.astype(jnp.bfloat16),
    }


def reference(residual, labels, loss_mask, norm_gain, embed_table):
    x_f32 = residual.astype(jnp.float32)
    inv_rms = lax.rsqrt(jnp.mean(x_f32 * x_f32, axis=-1, keepdims=True) + NORM_EPS)
    x_hat = x_f32 * inv_rms
    hidden = (x_hat * norm_gain).astype(jnp.bfloat16)
    mask_total = jnp.sum(loss_mask)
    tok_weight = loss_mask / mask_total
    col_ids = jnp.arange(VOCAB_PAD)[None, :]
    row_block = min(TOKENS, 256)
    n_blocks = TOKENS // row_block

    def block_step(grad_table, block_in):
        h_blk, lab_blk, w_blk = block_in
        logits = jnp.dot(h_blk, embed_table.T, preferred_element_type=jnp.float32) / LOGIT_SCALE
        logits = jnp.where(col_ids < VOCAB_REAL, logits, -jnp.inf)
        row_max = jnp.max(logits, axis=-1, keepdims=True)
        shifted = jnp.exp(logits - row_max)
        sum_exp = jnp.sum(shifted, axis=-1, keepdims=True)
        is_label = col_ids == lab_blk[:, None]
        target = jnp.sum(jnp.where(is_label, logits, 0.0), axis=-1)
        tok_loss = row_max[:, 0] + jnp.log(sum_exp[:, 0]) - target
        row_prob = shifted / sum_exp
        d_logits = (jnp.where(is_label, row_prob - 1.0, row_prob) * w_blk[:, None]).astype(jnp.bfloat16)
        d_hidden = jnp.dot(d_logits, embed_table, preferred_element_type=jnp.float32) / LOGIT_SCALE
        grad_table = grad_table + jnp.dot(d_logits.T, h_blk, preferred_element_type=jnp.float32) / LOGIT_SCALE
        return grad_table, (tok_loss, d_hidden)

    blocks = (hidden.reshape(n_blocks, row_block, DIM), labels.reshape(n_blocks, row_block), tok_weight.reshape(n_blocks, row_block))
    d_embed, (tok_loss, d_hidden) = lax.scan(block_step, jnp.zeros((VOCAB_PAD, DIM), jnp.float32), blocks)
    tok_loss = tok_loss.reshape(TOKENS)
    d_hidden = d_hidden.reshape(TOKENS, DIM)
    mean_loss = jnp.sum(loss_mask * tok_loss) / mask_total
    d_gain = jnp.sum(d_hidden * x_hat, axis=0)
    d_xhat = d_hidden * norm_gain
    d_residual = inv_rms * (d_xhat - x_hat * jnp.mean(d_xhat * x_hat, axis=-1, keepdims=True))
    return (mean_loss, d_residual, d_embed, d_gain)
```

```python
import jax
import jax.numpy as jnp
from jax import lax
from jax.experimental import pallas as pl
from jax.experimental.pallas import tpu as pltpu
from jax.sharding import PartitionSpec as P

VOCAB_REAL = 49155
LOGIT_SCALE = 6.0
NORM_EPS = 1e-6

MESH = pl.DeviceIdType.MESH
F32 = jnp.float32
BF16 = jnp.bfloat16

DEVS = 32
BIT = {"core": 0, "x": 1, "y": 2, "z1": 3, "z2": 4}
ORDERS = (("core", "x", "z1", "y", "z2"), ("core", "y", "z1", "x", "z2"))
STAGES = 5
ROWS = 16
CHUNK = DEVS * ROWS
HALF = 512
WSLOTS = 5


def block_of(order, dev):
    place = 0
    for name in ORDERS[order]:
        place = place * 2 + (dev >> BIT[name]) % 2
    return place


def make_kernel(chunks, vocab, vocab_pad, dim):
    tiles = [(lo, min(256, vocab_pad - lo)) for lo in range(0, vocab_pad, 256)]

    def kernel(x_ref, e_ref, g_ref, bias_ref, tbl_ref, dx_ref, de_ref, dgl_ref,
               e_s, x_s, h_s, z_s, dz_s, de_s, w_s, r0, r1, r2, r3, r4, d_s, st1, st2, p_s, loss_s, xo_s, fin1, fin2, dxo_s,
               e_sem, x_sem, s1s, s1r, s2s, s2r, ws, wr, f1s, f1r, f2s, f2r, o_sem):
        recv = (r0, r1, r2, r3, r4)
        me = lax.axis_index("vp")
        bits = {name: (me // (1 << k)) % 2 for name, k in BIT.items()}

        def flip(dev, name):
            return dev + (1 << BIT[name]) * (1 - 2 * bits[name])

        def plane_peer(r):
            dev = me
            for k, name in enumerate(("core", "x", "y")):
                if (r >> k) % 2:
                    dev = flip(dev, name)
            return dev

        def z_peer(r):
            dev = me
            for k, name in enumerate(("z1", "z2")):
                if (r >> k) % 2:
                    dev = flip(dev, name)
            return dev

        barrier = pltpu.get_barrier_semaphore()
        for r in range(1, 8):
            pl.semaphore_signal(barrier, inc=1, device_id=(plane_peer(r),), device_id_type=MESH)
        for r in range(1, 4):
            pl.semaphore_signal(barrier, inc=1, device_id=(z_peer(r),), device_id_type=MESH)

        def x_copy(c):
            return pltpu.make_async_copy(x_ref.at[:, c], x_s.at[lax.rem(c, 2)], x_sem.at[lax.rem(c, 2)])

        e_copy = pltpu.make_async_copy(e_ref, e_s.at[pl.ds(0, vocab)], e_sem.at[0])
        e_copy.start()
        x_copy(0).start()
        xo_copy = pltpu.make_async_copy(x_ref.at[me], xo_s, e_sem.at[1])
        xo_copy.start()
        e_s[pl.ds(vocab, vocab_pad - vocab), :] = jnp.zeros((vocab_pad - vocab, dim), BF16)
        de_s[...] = jnp.zeros_like(de_s)
        loss_s[...] = jnp.zeros_like(loss_s)
        e_copy.wait()
        first_pad = (VOCAB_REAL - (DEVS - 1) * vocab) // 16 * 16
        rows = lax.broadcasted_iota(jnp.int32, (vocab_pad - first_pad, 1), 0) + first_pad
        tail = e_s[pl.ds(first_pad, vocab_pad - first_pad), :]
        e_s[pl.ds(first_pad, vocab_pad - first_pad), :] = jnp.where(
            rows + me * vocab < VOCAB_REAL, tail, jnp.zeros_like(tail))
        pl.semaphore_wait(barrier, 10)

        def stat1_copy(c, r):
            slot = lax.rem(c, 2)
            return pltpu.make_async_remote_copy(
                st1.at[slot, 0], st1.at[slot, r], s1s.at[slot, r], s1r.at[slot, r],
                device_id=(plane_peer(r),), device_id_type=MESH)

        def stat2_copy(c, r):
            slot = lax.rem(c, 4)
            return pltpu.make_async_remote_copy(
                st2.at[slot, 0], st2.at[slot, r], s2s.at[slot, r], s2r.at[slot, r],
                device_id=(z_peer(r),), device_id_type=MESH)

        keep, give, peers = [], [], []
        for order in range(2):
            base, ks, gs, ps = 0, [], [], []
            size = DEVS
            for name in ORDERS[order]:
                size //= 2
                ks.append(base + bits[name] * size)
                gs.append(base + (1 - bits[name]) * size)
                ps.append(flip(me, name))
                base = ks[-1]
            keep.append(ks)
            give.append(gs)
            peers.append(ps)
        size_of = [DEVS >> (k + 1) for k in range(STAGES)]

        def rs_copy(k, c, order):
            slot = lax.rem(c, 2)
            return pltpu.make_async_remote_copy(
                w_s.at[lax.rem(c, WSLOTS), order, pl.ds(give[order][k], size_of[k])], recv[k].at[slot, order],
                ws.at[k, slot, order], wr.at[k, slot, order],
                device_id=(peers[order][k],), device_id_type=MESH)

        def advance(k, c):
            slot, wslot = lax.rem(c, 2), lax.rem(c, WSLOTS)
            for order in range(2):
                rs_copy(k, c, order).wait()
                mine = pl.ds(keep[order][k], size_of[k])
                total = w_s[wslot, order, mine] + recv[k][slot, order]
                if k < STAGES - 1:
                    w_s[wslot, order, mine] = total
                    rs_copy(k + 1, c, order).start()
                else:
                    d_s[pl.ds(pl.multiple_of(c * ROWS, ROWS), ROWS), order * HALF:(order + 1) * HALF] = total[0]

        def logits(c):
            x_copy(c).wait()

            @pl.when(c + 1 < chunks)
            def _():
                x_copy(c + 1).start()

            xv = x_s[lax.rem(c, 2)].reshape(CHUNK, dim).astype(F32)
            inv = lax.rsqrt(jnp.mean(xv * xv, axis=-1, keepdims=True) + NORM_EPS)
            hslot, zslot = lax.rem(c, 3), lax.rem(c, 2)
            h_s[hslot] = (xv * inv * g_ref[...]).astype(BF16)
            h = h_s[hslot]
            top = None
            for lo, width in tiles:
                z = lax.dot_general(h, e_s[lo:lo + width, :], (((1,), (1,)), ((), ())), preferred_element_type=F32)
                z = z * (1.0 / LOGIT_SCALE) + bias_ref[0:1, lo:lo + width]
                z_s[zslot, :, lo:lo + width] = z
                for i in range(0, width, 128):
                    part = z[:, i:i + 128]
                    top = part if top is None else jnp.maximum(top, part)
            m = jnp.max(top, axis=-1, keepdims=True)
            acc = None
            for lo, width in tiles:
                p = jnp.exp(z_s[zslot, :, lo:lo + width] - m)
                for i in range(0, width, 128):
                    part = p[:, i:i + 128]
                    acc = part if acc is None else acc + part
            s = jnp.sum(acc, axis=-1, keepdims=True)
            lane = lax.broadcasted_iota(jnp.int32, (CHUNK, 128), 1)
            pair = jnp.where(lane == 0, m, s).T
            slot = lax.rem(c, 2)
            for i in range(4):
                st1[slot, 0, i:i + 1, :] = pair[0:1, i * 128:(i + 1) * 128]
                st1[slot, 0, 4 + i:5 + i, :] = pair[1:2, i * 128:(i + 1) * 128]
            for r in range(1, 8):
                stat1_copy(c, r).start()

        def merge(ref, slot, n):
            ms = [ref[slot, r, 0:4, :] for r in range(n)]
            ss = [ref[slot, r, 4:8, :] for r in range(n)]
            m = ms[0]
            for v in ms[1:]:
                m = jnp.maximum(m, v)
            s = ss[0] * jnp.exp(ms[0] - m)
            for a, b in zip(ms[1:], ss[1:]):
                s = s + b * jnp.exp(a - m)
            return m, s

        def stats1(c):
            for r in range(1, 8):
                stat1_copy(c, r).wait()
            m, s = merge(st1, lax.rem(c, 2), 8)
            slot = lax.rem(c, 4)
            st2[slot, 0, 0:4, :] = m
            st2[slot, 0, 4:8, :] = s
            for r in range(1, 4):
                stat2_copy(c, r).start()

        def grads(c):
            for r in range(1, 4):
                stat2_copy(c, r).wait()
            m, s = merge(st2, lax.rem(c, 4), 4)
            lse = m + jnp.log(s)
            p_s[...] = tbl_ref[c]
            for i in range(4):
                p_s[2:3, i * 128:(i + 1) * 128] = lse[i:i + 1, :]
            cols = p_s[...].T
            label, weight, lse_col = cols[:, 0:1], cols[:, 1:2], cols[:, 2:3]
            zslot = lax.rem(c, 2)
            hit_sum = None
            for lo, width in tiles:
                z = z_s[zslot, :, lo:lo + width]
                p = jnp.exp(z - lse_col)
                col = lax.broadcasted_iota(jnp.int32, (1, width), 1).astype(F32) + float(lo)
                hit = col == label
                dz_s[:, lo:lo + width] = (jnp.where(hit, p - 1.0, p) * weight).astype(BF16)
                hz = jnp.where(hit, z, 0.0)
                for i in range(0, width, 128):
                    part = hz[:, i:i + 128]
                    hit_sum = part if hit_sum is None else hit_sum + part
            row = lax.broadcasted_iota(jnp.int32, (CHUNK, 1), 0)
            own = (row >= me * ROWS) & (row < me * ROWS + ROWS)
            term = weight * (jnp.where(own, lse_col, 0.0) - jnp.sum(hit_sum, axis=-1, keepdims=True))
            loss_s[...] += jnp.sum(term, axis=0, keepdims=True)
            wslot = lax.rem(c, WSLOTS)
            for order in range(2):
                dh = jnp.dot(dz_s[...], e_s[:, order * HALF:(order + 1) * HALF], preferred_element_type=F32)
                for dev in range(DEVS):
                    w_s[wslot, order, block_of(order, dev)] = dh[dev * ROWS:(dev + 1) * ROWS, :]
                rs_copy(0, c, order).start()

        def table_grad(c):
            h = h_s[lax.rem(c, 3)]
            for lo, width in tiles:
                de_s[lo:lo + width, :] += lax.dot_general(
                    dz_s[:, lo:lo + width], h, (((0,), (0,)), ((), ())), preferred_element_type=F32)

        def step(i, carry):
            @pl.when(i < chunks)
            def _():
                logits(i)

            @pl.when((i >= 2) & (i < chunks + 2))
            def _():
                table_grad(i - 2)

            @pl.when(i < chunks)
            def _():
                stats1(i)

            for k in reversed(range(STAGES)):
                @pl.when((i >= k + 2) & (i < chunks + k + 2))
                def _(k=k):
                    advance(k, i - k - 2)

            @pl.when((i >= 1) & (i < chunks + 1))
            def _():
                grads(i - 1)

            return carry

        lax.fori_loop(0, chunks + STAGES + 1, step, 0)

        de_copy = pltpu.make_async_copy(de_s.at[pl.ds(0, vocab)], de_ref, o_sem.at[0])
        de_copy.start()

        xo_copy.wait()
        xv = xo_s[...].reshape(chunks * ROWS, dim).astype(F32)
        inv = lax.rsqrt(jnp.mean(xv * xv, axis=-1, keepdims=True) + NORM_EPS)
        xh = xv * inv
        dh = d_s[...] * (1.0 / LOGIT_SCALE)
        gain = jnp.sum(dh * xh, axis=0, keepdims=True)
        zid, pid = me // 8, lax.rem(me, 8)
        for i in range(8):
            fin1[pid, i:i + 1, :] = gain[:, i * 128:(i + 1) * 128]
        fin1[pid, 8:16, :] = jnp.broadcast_to(loss_s[0:1, :], (8, 128))

        def fin_copy(buf, at, r, ss, rs, dev):
            return pltpu.make_async_remote_copy(
                buf.at[at], buf.at[at], ss.at[r], rs.at[r], device_id=(dev,), device_id_type=MESH)

        first = [fin_copy(fin1, pid, r, f1s, f1r, plane_peer(r)) for r in range(1, 8)]
        for c in first:
            c.start()
        u = dh * g_ref[...]
        dxo_s[...] = inv * (u - xh * jnp.mean(u * xh, axis=-1, keepdims=True))
        dx_copy = pltpu.make_async_copy(dxo_s, dx_ref, o_sem.at[1])
        dx_copy.start()
        for c in first:
            c.wait()
        total = fin1[0]
        for i in range(1, 8):
            total = total + fin1[i]
        fin2[zid] = total
        second = [fin_copy(fin2, zid, r, f2s, f2r, z_peer(r)) for r in range(1, 4)]
        for c in second:
            c.start()
        for c in second:
            c.wait()
        total = fin2[0]
        for i in range(1, 4):
            total = total + fin2[i]
        dgl_ref[...] = total
        de_copy.wait()
        dx_copy.wait()

    return kernel


def solution(mesh):
    def local_step(residual, labels, loss_mask, norm_gain, table_shard):
        tokens, dim = residual.shape
        vocab = table_shard.shape[0]
        vocab_pad = -(-vocab // 128) * 128
        chunks = tokens // CHUNK
        me = lax.axis_index("vp")
        ids = me * vocab + lax.broadcasted_iota(jnp.int32, (8, vocab_pad), 1)
        live = (ids < VOCAB_REAL) & (lax.broadcasted_iota(jnp.int32, (8, vocab_pad), 1) < vocab)
        bias = jnp.where(live, 0.0, -jnp.inf).astype(F32)
        local = (labels - me * vocab)
        local = jnp.where((local >= 0) & (local < vocab), local, -1).astype(F32)
        weight = loss_mask / jnp.sum(loss_mask)

        def by_chunk(v):
            return v.reshape(DEVS, chunks, ROWS).transpose(1, 0, 2).reshape(chunks, 1, CHUNK)

        tbl = jnp.concatenate([by_chunk(local), by_chunk(weight), jnp.zeros((chunks, 6, CHUNK), F32)], axis=1)
        anyspec = pl.BlockSpec(memory_space=pl.ANY)
        vspec = pl.BlockSpec(memory_space=pltpu.VMEM)
        sems = pltpu.SemaphoreType.DMA
        dx, de, dgl = pl.pallas_call(
            make_kernel(chunks, vocab, vocab_pad, dim),
            out_shape=(jax.ShapeDtypeStruct((chunks * ROWS, dim), F32),
                       jax.ShapeDtypeStruct((vocab, dim), F32),
                       jax.ShapeDtypeStruct((16, 128), F32)),
            in_specs=[anyspec, anyspec, vspec, vspec, vspec],
            out_specs=(anyspec, anyspec, vspec),
            scratch_shapes=[
                pltpu.VMEM((vocab_pad, dim), BF16),
                pltpu.VMEM((2, DEVS, ROWS, dim), BF16),
                pltpu.VMEM((3, CHUNK, dim), BF16),
                pltpu.VMEM((2, CHUNK, vocab_pad), F32),
                pltpu.VMEM((CHUNK, vocab_pad), BF16),
                pltpu.VMEM((vocab_pad, dim), F32),
                pltpu.VMEM((WSLOTS, 2, DEVS, ROWS, HALF), F32),
                *[pltpu.VMEM((2, 2, DEVS >> (k + 1), ROWS, HALF), F32) for k in range(STAGES)],
                pltpu.VMEM((chunks * ROWS, dim), F32),
                pltpu.VMEM((2, 8, 8, 128), F32),
                pltpu.VMEM((4, 4, 8, 128), F32),
                pltpu.VMEM((8, CHUNK), F32),
                pltpu.VMEM((8, 128), F32),
                pltpu.VMEM((chunks, ROWS, dim), BF16),
                pltpu.VMEM((8, 16, 128), F32),
                pltpu.VMEM((4, 16, 128), F32),
                pltpu.VMEM((chunks * ROWS, dim), F32),
                sems((2,)), sems((2,)),
                sems((2, 8)), sems((2, 8)), sems((4, 4)), sems((4, 4)),
                sems((STAGES, 2, 2)), sems((STAGES, 2, 2)),
                sems((8,)), sems((8,)), sems((4,)), sems((4,)), sems((2,)),
            ],
            compiler_params=pltpu.CompilerParams(collective_id=0, has_side_effects=True, vmem_limit_bytes=62 * 1024 * 1024),
        )(residual.reshape(DEVS, chunks, ROWS, dim), table_shard, norm_gain.reshape(1, dim), bias, tbl)
        return dgl[8, 0], dx, de / LOGIT_SCALE, dgl[:8].reshape(dim)

    return jax.shard_map(
        local_step, mesh=mesh, in_specs=(P(), P(), P(), P(), P("vp", None)),
        out_specs=(P(), P("vp", None), P("vp", None), P()), check_vma=False)
```

```python
import jax
import jax.numpy as jnp
from jax import lax
from jax.experimental import pallas as pl
from jax.experimental.pallas import tpu as pltpu
from jax.sharding import PartitionSpec as P

VOCAB_REAL = 49155
LOGIT_SCALE = 6.0
NORM_EPS = 1e-6

MESH = pl.DeviceIdType.MESH
F32 = jnp.float32
BF16 = jnp.bfloat16

DEVS = 32
BIT = {"core": 0, "x": 1, "y": 2, "z1": 3, "z2": 4}
ORDERS = (("core", "x", "z1", "y", "z2"), ("core", "y", "z1", "x", "z2"))
STAGES = 5
ROWS = 16
CHUNK = DEVS * ROWS
HALF = 512
WSLOTS = 7
LAG = 3
WAIT_AT = (4, 6, 8, 9, 10)
SLOTS = (2, 4, 4, 2, 2)
XSLOTS, HSLOTS, ZSLOTS = 2, 5, 4


def block_of(order, dev):
    place = 0
    for name in ORDERS[order]:
        place = place * 2 + (dev >> BIT[name]) % 2
    return place


def weave(first, second):
    order = [((n + 0.5) / len(first), 0, n) for n in range(len(first))]
    order += [((n + 0.5) / len(second), 1, n) for n in range(len(second))]
    for _, which, n in sorted(order):
        (first, second)[which][n]()


def make_kernel(chunks, vocab, vocab_pad, dim):
    tiles = [(lo, min(256, vocab_pad - lo)) for lo in range(0, vocab_pad, 256)]
    row_tiles = [(lo, 256) for lo in range(0, vocab - 511, 256)]
    row_tiles.append((row_tiles[-1][0] + 256, vocab - row_tiles[-1][0] - 256))
    first_pad = (VOCAB_REAL - (DEVS - 1) * vocab) // 16 * 16
    blocks = 8
    rows_in = CHUNK // blocks
    devs_in = DEVS // blocks

    def kernel(x_ref, e_ref, g_ref, tbl_ref, dx_ref, de_ref, dg_ref, loss_ref,
               bias_s, e_s, x_s, h_s, z_s, dz_s, w_s, r0, r1, r2, r3, r4, d_s, st1, st2, p_s, loss_s, xo_s, fin1, fin2, dxo_s, late_s,
               e_sem, x_sem, s1s, s1r, s2s, s2r, ws, wr, f1s, f1r, f2s, f2r, o_sem):
        recv = (r0, r1, r2, r3, r4)
        me = lax.axis_index("vp")
        bits = {name: (me // (1 << k)) % 2 for name, k in BIT.items()}

        def flip(dev, name):
            return dev + (1 << BIT[name]) * (1 - 2 * bits[name])

        def plane_peer(r):
            dev = me
            for k, name in enumerate(("core", "x", "y")):
                if (r >> k) % 2:
                    dev = flip(dev, name)
            return dev

        def z_peer(r):
            dev = me
            for k, name in enumerate(("z1", "z2")):
                if (r >> k) % 2:
                    dev = flip(dev, name)
            return dev

        barrier = pltpu.get_barrier_semaphore()
        for r in range(1, 8):
            pl.semaphore_signal(barrier, inc=1, device_id=(plane_peer(r),), device_id_type=MESH)
        for r in range(1, 4):
            pl.semaphore_signal(barrier, inc=1, device_id=(z_peer(r),), device_id_type=MESH)

        def x_copy(c):
            slot = lax.rem(c, XSLOTS)
            return pltpu.make_async_copy(x_ref.at[:, c], x_s.at[slot], x_sem.at[slot])

        e_copy = pltpu.make_async_copy(e_ref, e_s.at[pl.ds(0, vocab)], e_sem.at[0])
        x_copy(0).start()
        e_copy.start()
        x_copy(1).start()
        xo_copy = pltpu.make_async_copy(x_ref.at[me], xo_s, e_sem.at[1])
        xo_copy.start()
        e_s[pl.ds(vocab, vocab_pad - vocab), :] = jnp.zeros((vocab_pad - vocab, dim), BF16)
        ids = lax.broadcasted_iota(jnp.int32, (8, vocab_pad), 1)
        live = (ids < vocab) & (ids + me * vocab < VOCAB_REAL)
        bias_s[...] = jnp.where(live, 0.0, -jnp.inf).astype(F32)
        halves = tbl_ref[...] * 0.5
        total_mask = jnp.sum(jnp.sum(2.0 * (halves - jnp.floor(halves)), axis=1, keepdims=True), axis=0, keepdims=True)
        unit = 1.0 / total_mask
        first_id = (me * vocab).astype(F32)
        loss_s[...] = jnp.zeros_like(loss_s)

        def stat1_copy(c, r):
            slot = lax.rem(c, 4)
            return pltpu.make_async_remote_copy(
                st1.at[slot, 0], st1.at[slot, r], s1s.at[slot, r], s1r.at[slot, r],
                device_id=(plane_peer(r),), device_id_type=MESH)

        def stat2_copy(c, r):
            slot = lax.rem(c, 4)
            return pltpu.make_async_remote_copy(
                st2.at[slot, 0], st2.at[slot, r], s2s.at[slot, r], s2r.at[slot, r],
                device_id=(z_peer(r),), device_id_type=MESH)

        keep, give, peers = [], [], []
        for order in range(2):
            base, ks, gs, ps = 0, [], [], []
            size = DEVS
            for name in ORDERS[order]:
                size //= 2
                ks.append(base + bits[name] * size)
                gs.append(base + (1 - bits[name]) * size)
                ps.append(flip(me, name))
                base = ks[-1]
            keep.append(ks)
            give.append(gs)
            peers.append(ps)
        size_of = [DEVS >> (k + 1) for k in range(STAGES)]

        def rs_copy(k, c, order):
            slot = lax.rem(c, SLOTS[k])
            return pltpu.make_async_remote_copy(
                w_s.at[lax.rem(c, WSLOTS), order, pl.ds(give[order][k], size_of[k])], recv[k].at[slot, order],
                ws.at[k, slot, order], wr.at[k, slot, order],
                device_id=(peers[order][k],), device_id_type=MESH)

        def advance(k, c):
            slot, wslot = lax.rem(c, SLOTS[k]), lax.rem(c, WSLOTS)
            for order in range(2):
                rs_copy(k, c, order).wait()
                mine = pl.ds(keep[order][k], size_of[k])
                total = w_s[wslot, order, mine] + recv[k][slot, order]
                if k < STAGES - 1:
                    w_s[wslot, order, mine] = total
                    rs_copy(k + 1, c, order).start()
                else:
                    d_s[pl.ds(pl.multiple_of(c * ROWS, ROWS), ROWS), order * HALF:(order + 1) * HALF] = total[0]

        def norm_units(c):
            xslot, hslot = lax.rem(c, XSLOTS), lax.rem(c, HSLOTS)

            def unit_of(b):
                def run():
                    xv = x_s[xslot, b * devs_in:(b + 1) * devs_in].reshape(rows_in, dim).astype(F32)
                    inv = lax.rsqrt(jnp.mean(xv * xv, axis=-1, keepdims=True) + NORM_EPS)
                    h_s[hslot, b * rows_in:(b + 1) * rows_in, :] = (xv * inv * g_ref[...]).astype(BF16)
                return run
            return [unit_of(b) for b in range(blocks)]

        def logit_units(c):
            hslot, zslot = lax.rem(c, HSLOTS), lax.rem(c, ZSLOTS)

            def unit_of(lo, width):
                def run():
                    z = lax.dot_general(h_s[hslot], e_s[lo:lo + width, :], (((1,), (1,)), ((), ())), preferred_element_type=F32)
                    z = z * (1.0 / LOGIT_SCALE)
                    if lo + width > first_pad:
                        z = z + bias_s[0:1, lo:lo + width]
                    z_s[zslot, :, lo:lo + width] = z
                return run
            return [unit_of(lo, width) for lo, width in tiles]

        def sum_units(c, out):
            zslot = lax.rem(c, ZSLOTS)

            def unit_of(b):
                def run():
                    rows = slice(b * rows_in, (b + 1) * rows_in)
                    top = z_s[zslot, rows, 0:128]
                    for lo in range(128, vocab_pad, 128):
                        top = jnp.maximum(top, z_s[zslot, rows, lo:lo + 128])
                    m = jnp.max(top, axis=-1, keepdims=True)
                    acc = jnp.exp(z_s[zslot, rows, 0:128] - m)
                    for lo in range(128, vocab_pad, 128):
                        acc = acc + jnp.exp(z_s[zslot, rows, lo:lo + 128] - m)
                    s = jnp.sum(acc, axis=-1, keepdims=True)
                    lane = lax.broadcasted_iota(jnp.int32, (rows_in, 128), 1)
                    out.append(jnp.where(lane == 0, m, s))
                return run
            return [unit_of(b) for b in range(blocks)]

        def send_stats(c, parts):
            slot = lax.rem(c, 4)
            per = 128 // rows_in
            for i in range(4):
                pair = jnp.concatenate(parts[i * per:(i + 1) * per], axis=0).T
                st1[slot, 0, i:i + 1, :] = pair[0:1, :]
                st1[slot, 0, 4 + i:5 + i, :] = pair[1:2, :]
            for r in range(1, 8):
                stat1_copy(c, r).start()

        def merge(ref, slot, n):
            ms = [ref[slot, r, 0:4, :] for r in range(n)]
            ss = [ref[slot, r, 4:8, :] for r in range(n)]
            m = ms[0]
            for v in ms[1:]:
                m = jnp.maximum(m, v)
            s = ss[0] * jnp.exp(ms[0] - m)
            for a, b in zip(ms[1:], ss[1:]):
                s = s + b * jnp.exp(a - m)
            return m, s

        def stats1(c):
            for r in range(1, 8):
                stat1_copy(c, r).wait()
            m, s = merge(st1, lax.rem(c, 4), 8)
            slot = lax.rem(c, 4)
            st2[slot, 0, 0:4, :] = m
            st2[slot, 0, 4:8, :] = s
            for r in range(1, 4):
                stat2_copy(c, r).start()

        def token_columns(c):
            for r in range(1, 4):
                stat2_copy(c, r).wait()
            m, s = merge(st2, lax.rem(c, 4), 4)
            lse = m + jnp.log(s)
            code = tbl_ref[pl.ds(c, 1), :] * 0.5
            label = jnp.floor(code)
            local = label - first_id
            p_s[0:1, :] = jnp.where(local < float(vocab), local, -1.0)
            p_s[1:2, :] = 2.0 * (code - label) * unit
            for i in range(4):
                p_s[2:3, i * 128:(i + 1) * 128] = lse[i:i + 1, :]
            return p_s[...].T

        def dz_units(c, cols):
            zslot = lax.rem(c, ZSLOTS)

            def unit_of(b):
                def run():
                    rows = slice(b * rows_in, (b + 1) * rows_in)
                    label, weight, lse = (cols[rows, k:k + 1] for k in range(3))
                    hit_sum = jnp.zeros((rows_in, 128), F32)
                    for lo, width in tiles:
                        z = z_s[zslot, rows, lo:lo + width]
                        p = jnp.exp(z - lse)
                        col = lax.broadcasted_iota(jnp.int32, (1, width), 1).astype(F32) + float(lo)
                        hit = col == label
                        dz_s[rows, lo:lo + width] = (jnp.where(hit, p - 1.0, p) * weight).astype(BF16)
                        hz = jnp.where(hit, z, 0.0)
                        for i in range(0, width, 128):
                            hit_sum = hit_sum + hz[:, i:i + 128]
                    row = lax.broadcasted_iota(jnp.int32, (rows_in, 1), 0) + b * rows_in
                    own = (row >= me * ROWS) & (row < me * ROWS + ROWS)
                    term = weight * (jnp.where(own, lse, 0.0) - jnp.sum(hit_sum, axis=-1, keepdims=True))
                    loss_s[...] += jnp.sum(term, axis=0, keepdims=True)
                return run
            return [unit_of(b) for b in range(blocks)]

        def dh_units(c):
            wslot = lax.rem(c, WSLOTS)

            def unit_of(n):
                def run():
                    order, lo = divmod(n * 256, HALF)
                    dh = jnp.dot(dz_s[...], e_s[:, n * 256:(n + 1) * 256], preferred_element_type=F32)
                    for dev in range(DEVS):
                        w_s[wslot, order, block_of(order, dev), :, lo:lo + 256] = dh[dev * ROWS:(dev + 1) * ROWS, :]
                return run
            return [unit_of(n) for n in range(dim // 256)]

        def table_units(c):
            hslot = lax.rem(c, HSLOTS)

            def unit_of(lo, width):
                def run():
                    de_ref[lo:lo + width, :] += lax.dot_general(
                        dz_s[:, lo:lo + width], h_s[hslot], (((0,), (0,)), ((), ())), preferred_element_type=F32)
                return run
            return [unit_of(lo, width) for lo, width in row_tiles]

        def last_gain(c):
            xslot, wslot = lax.rem(c, XSLOTS), lax.rem(c, WSLOTS)
            gains = [jnp.zeros((ROWS, HALF), F32) for _ in range(2)]
            for dev in range(DEVS):
                xv = x_s[xslot, dev].astype(F32)
                xh = xv * lax.rsqrt(jnp.mean(xv * xv, axis=-1, keepdims=True) + NORM_EPS)
                for order in range(2):
                    gains[order] = gains[order] + xh[:, order * HALF:(order + 1) * HALF] * w_s[wslot, order, block_of(order, dev)]
            for order in range(2):
                late_s[0:1, order * HALF:(order + 1) * HALF] = jnp.sum(gains[order], axis=0, keepdims=True) * (1.0 / LOGIT_SCALE)

        def block_a(i, norm, table):
            for run in (table_units(i - LAG - 1) if table else []) + (norm_units(i + 1) if norm else []):
                run()

        def block_b(i, fwd, bwd):
            cols = token_columns(i - LAG) if bwd else None
            parts = []
            unit_lists = {"L": logit_units(i) if fwd else [], "Z": dz_units(i - LAG, cols) if bwd else [],
                          "D": dh_units(i - LAG) if bwd else [], "S": sum_units(i, parts) if fwd else []}
            for name in "LZDS":
                for run in unit_lists[name]:
                    run()
            if bwd:
                for order in range(2):
                    rs_copy(0, i - LAG, order).start()
            if fwd:
                send_stats(i, parts)

        def either(low, high, i, first, run):
            a, b = i < first, (i >= low) & (i < high)
            pl.when(a & b)(lambda: run(i, True, True))
            pl.when(a & jnp.logical_not(b))(lambda: run(i, True, False))
            pl.when(jnp.logical_not(a) & b)(lambda: run(i, False, True))

        zid, pid = me // 8, lax.rem(me, 8)

        def own_rows(lo, n):
            xv = xo_s[lo // ROWS:(lo + n) // ROWS].reshape(n, dim).astype(F32)
            inv = lax.rsqrt(jnp.mean(xv * xv, axis=-1, keepdims=True) + NORM_EPS)
            xh = xv * inv
            dh = d_s[lo:lo + n, :] * (1.0 / LOGIT_SCALE)
            u = dh * g_ref[...]
            dxo_s[lo:lo + n, :] = inv * (u - xh * jnp.mean(u * xh, axis=-1, keepdims=True))
            return dh * xh

        def fin_copy(buf, at, r, ss, rs, dev):
            return pltpu.make_async_remote_copy(
                buf.at[at], buf.at[at], ss.at[r], rs.at[r], device_id=(dev,), device_id_type=MESH)

        first = [fin_copy(fin1, pid, r, f1s, f1r, plane_peer(r)) for r in range(1, 8)]
        second = [fin_copy(fin2, zid, r, f2s, f2r, z_peer(r)) for r in range(1, 4)]

        def early_rows():
            gain = jnp.sum(own_rows(0, (chunks - 1) * ROWS), axis=0, keepdims=True) + late_s[0:1, :]
            for i in range(8):
                fin1[pid, i:i + 1, :] = gain[:, i * 128:(i + 1) * 128]
            fin1[pid, 8:16, :] = jnp.broadcast_to(loss_s[0:1, :], (8, 128))
            for c in first:
                c.start()

        def merge_plane():
            for c in first:
                c.wait()
            total = fin1[0]
            for i in range(1, 8):
                total = total + fin1[i]
            fin2[zid] = total
            for c in second:
                c.start()

        x_copy(0).wait()
        for run in norm_units(0):
            run()
        de_ref[...] = jnp.zeros_like(de_ref)
        e_copy.wait()
        rows = lax.broadcasted_iota(jnp.int32, (vocab_pad - first_pad, 1), 0) + first_pad
        tail = e_s[pl.ds(first_pad, vocab_pad - first_pad), :]
        e_s[pl.ds(first_pad, vocab_pad - first_pad), :] = jnp.where(
            rows + me * vocab < VOCAB_REAL, tail, jnp.zeros_like(tail))
        xo_copy.wait()
        pl.semaphore_wait(barrier, 10)

        def step(i, carry):
            @pl.when((i >= 0) & (i + 2 < chunks))
            def _():
                x_copy(i + 2).start()

            @pl.when(i + 1 < chunks)
            def _():
                x_copy(i + 1).wait()

            either(LAG + 1, chunks + LAG + 1, i, chunks - 1, block_a)

            for k in reversed(range(STAGES)):
                @pl.when((i >= WAIT_AT[k]) & (i < chunks + WAIT_AT[k]))
                def _(k=k):
                    advance(k, i - WAIT_AT[k])

            either(LAG, chunks + LAG, i, chunks, block_b)

            @pl.when((i >= 1) & (i < chunks + 1))
            def _():
                stats1(i - 1)

            @pl.when(i == chunks + LAG - 1)
            def _():
                last_gain(chunks - 1)

            @pl.when(i == chunks - 2 + WAIT_AT[-1])
            def _():
                early_rows()

            return carry

        lax.fori_loop(0, chunks - 1 + WAIT_AT[-1], step, 0)

        last = chunks - 1
        merge_plane()
        advance(STAGES - 1, last)
        own_rows(last * ROWS, ROWS)
        dx_copy = pltpu.make_async_copy(dxo_s, dx_ref, o_sem.at[1])
        dx_copy.start()
        for c in second:
            c.wait()
        total = fin2[0]
        for i in range(1, 4):
            total = total + fin2[i]
        for i in range(8):
            dg_ref[0:1, i * 128:(i + 1) * 128] = total[i:i + 1, :]
        loss_ref[...] = total[8:16, :]
        dx_copy.wait()

    return kernel


def solution(mesh):
    def local_step(residual, labels, loss_mask, norm_gain, table_shard):
        tokens, dim = residual.shape
        vocab = table_shard.shape[0]
        vocab_pad = -(-vocab // 128) * 128
        chunks = tokens // CHUNK
        def by_chunk(v):
            return v.reshape(DEVS, chunks, ROWS).transpose(1, 0, 2).reshape(chunks, CHUNK)

        tbl = by_chunk((2 * labels + loss_mask.astype(jnp.int32)).astype(F32))
        anyspec = pl.BlockSpec(memory_space=pl.ANY)
        vspec = pl.BlockSpec(memory_space=pltpu.VMEM)
        sems = pltpu.SemaphoreType.DMA
        dx, de, dg, loss = pl.pallas_call(
            make_kernel(chunks, vocab, vocab_pad, dim),
            out_shape=(jax.ShapeDtypeStruct((chunks * ROWS, dim), F32),
                       jax.ShapeDtypeStruct((vocab, dim), F32),
                       jax.ShapeDtypeStruct((1, dim), F32),
                       jax.ShapeDtypeStruct((8, 128), F32)),
            in_specs=[anyspec, anyspec, vspec, vspec],
            out_specs=(anyspec, vspec, vspec, vspec),
            scratch_shapes=[
                pltpu.VMEM((8, vocab_pad), F32),
                pltpu.VMEM((vocab_pad, dim), BF16),
                pltpu.VMEM((XSLOTS, DEVS, ROWS, dim), BF16),
                pltpu.VMEM((HSLOTS, CHUNK, dim), BF16),
                pltpu.VMEM((ZSLOTS, CHUNK, vocab_pad), F32),
                pltpu.VMEM((CHUNK, vocab_pad), BF16),
                pltpu.VMEM((WSLOTS, 2, DEVS, ROWS, HALF), F32),
                *[pltpu.VMEM((SLOTS[k], 2, DEVS >> (k + 1), ROWS, HALF), F32) for k in range(STAGES)],
                pltpu.VMEM((chunks * ROWS, dim), F32),
                pltpu.VMEM((4, 8, 8, 128), F32),
                pltpu.VMEM((4, 4, 8, 128), F32),
                pltpu.VMEM((8, CHUNK), F32),
                pltpu.VMEM((8, 128), F32),
                pltpu.VMEM((chunks, ROWS, dim), BF16),
                pltpu.VMEM((8, 16, 128), F32),
                pltpu.VMEM((4, 16, 128), F32),
                pltpu.VMEM((chunks * ROWS, dim), F32),
                pltpu.VMEM((8, dim), F32),
                sems((2,)), sems((2,)),
                sems((4, 8)), sems((4, 8)), sems((4, 4)), sems((4, 4)),
                sems((STAGES, 4, 2)), sems((STAGES, 4, 2)),
                sems((8,)), sems((8,)), sems((4,)), sems((4,)), sems((2,)),
            ],
            compiler_params=pltpu.CompilerParams(collective_id=0, has_side_effects=True, vmem_limit_bytes=62 * 1024 * 1024),
        )(residual.reshape(DEVS, chunks, ROWS, dim), table_shard, norm_gain.reshape(1, dim), tbl)
        return loss[0, 0], dx, de / LOGIT_SCALE, dg.reshape(dim)

    return jax.shard_map(
        local_step, mesh=mesh, in_specs=(P(), P(), P(), P(), P("vp", None)),
        out_specs=(P(), P("vp", None), P("vp", None), P()), check_vma=False)
```

```python
import jax
import jax.numpy as jnp
from jax import lax
from jax.experimental import pallas as pl
from jax.experimental.pallas import tpu as pltpu
from jax.sharding import PartitionSpec as P

VOCAB_REAL = 49155
LOGIT_SCALE = 6.0
NORM_EPS = 1e-6

MESH = pl.DeviceIdType.MESH
F32 = jnp.float32
BF16 = jnp.bfloat16

DEVS = 32
BIT = {"core": 0, "x": 1, "y": 2, "z1": 3, "z2": 4}
ORDERS = (("core", "x", "z1", "y", "z2"), ("core", "y", "z1", "x", "z2"))
STAGES = 5
ROWS = 16
CHUNK = DEVS * ROWS
HALF = 512
WSLOTS = 7
LAG = 3
WAIT_AT = (4, 6, 8, 9, 10)
SLOTS = (2, 4, 4, 2, 2)
XSLOTS, HSLOTS, ZSLOTS = 2, 5, 4


def block_of(order, dev):
    place = 0
    for name in ORDERS[order]:
        place = place * 2 + (dev >> BIT[name]) % 2
    return place


def weave(first, second):
    order = [((n + 0.5) / len(first), 0, n) for n in range(len(first))]
    order += [((n + 0.5) / len(second), 1, n) for n in range(len(second))]
    for _, which, n in sorted(order):
        (first, second)[which][n]()


def make_kernel(chunks, vocab, vocab_pad, dim):
    tiles = [(lo, min(256, vocab_pad - lo)) for lo in range(0, vocab_pad, 256)]
    row_tiles = [(lo, 256) for lo in range(0, vocab - 511, 256)]
    row_tiles.append((row_tiles[-1][0] + 256, vocab - row_tiles[-1][0] - 256))
    first_pad = (VOCAB_REAL - (DEVS - 1) * vocab) // 16 * 16
    blocks = 8
    rows_in = CHUNK // blocks
    devs_in = DEVS // blocks

    def kernel(x_ref, e_ref, g_ref, tbl_ref, dx_ref, de_ref, fin_ref,
               de_s, bias_s, e_s, x_s, h_s, z_s, dz_s, w_s, r0, r1, r2, r3, r4, d_s, st1, st2, p_s, loss_s, xo_s, fin1, fin2, dxo_s, late_s,
               e_sem, x_sem, s1s, s1r, s2s, s2r, ws, wr, f1s, f1r, f2s, f2r, o_sem):
        recv = (r0, r1, r2, r3, r4)
        me = lax.axis_index("vp")
        bits = {name: (me // (1 << k)) % 2 for name, k in BIT.items()}

        def flip(dev, name):
            return dev + (1 << BIT[name]) * (1 - 2 * bits[name])

        def plane_peer(r):
            dev = me
            for k, name in enumerate(("core", "x", "y")):
                if (r >> k) % 2:
                    dev = flip(dev, name)
            return dev

        def z_peer(r):
            dev = me
            for k, name in enumerate(("z1", "z2")):
                if (r >> k) % 2:
                    dev = flip(dev, name)
            return dev

        barrier = pltpu.get_barrier_semaphore()
        for r in range(1, 8):
            pl.semaphore_signal(barrier, inc=1, device_id=(plane_peer(r),), device_id_type=MESH)
        for r in range(1, 4):
            pl.semaphore_signal(barrier, inc=1, device_id=(z_peer(r),), device_id_type=MESH)

        def x_copy(c):
            slot = lax.rem(c, XSLOTS)
            return pltpu.make_async_copy(x_ref.at[:, c], x_s.at[slot], x_sem.at[slot])

        e_copy = pltpu.make_async_copy(e_ref, e_s.at[pl.ds(0, vocab)], e_sem.at[0])
        x_copy(0).start()
        e_copy.start()
        x_copy(1).start()
        xo_copy = pltpu.make_async_copy(x_ref.at[me], xo_s, e_sem.at[1])
        xo_copy.start()
        e_s[pl.ds(vocab, vocab_pad - vocab), :] = jnp.zeros((vocab_pad - vocab, dim), BF16)
        ids = lax.broadcasted_iota(jnp.int32, (8, vocab_pad), 1)
        live = (ids < vocab) & (ids + me * vocab < VOCAB_REAL)
        bias_s[...] = jnp.where(live, 0.0, -jnp.inf).astype(F32)
        halves = tbl_ref[...] * 0.5
        total_mask = jnp.sum(jnp.sum(2.0 * (halves - jnp.floor(halves)), axis=1, keepdims=True), axis=0, keepdims=True)
        unit = 1.0 / total_mask
        first_id = (me * vocab).astype(F32)
        loss_s[...] = jnp.zeros_like(loss_s)

        def stat1_copy(c, r):
            slot = lax.rem(c, 4)
            return pltpu.make_async_remote_copy(
                st1.at[slot, 0], st1.at[slot, r], s1s.at[slot, r], s1r.at[slot, r],
                device_id=(plane_peer(r),), device_id_type=MESH)

        def stat2_copy(c, r):
            slot = lax.rem(c, 4)
            return pltpu.make_async_remote_copy(
                st2.at[slot, 0], st2.at[slot, r], s2s.at[slot, r], s2r.at[slot, r],
                device_id=(z_peer(r),), device_id_type=MESH)

        keep, give, peers = [], [], []
        for order in range(2):
            base, ks, gs, ps = 0, [], [], []
            size = DEVS
            for name in ORDERS[order]:
                size //= 2
                ks.append(base + bits[name] * size)
                gs.append(base + (1 - bits[name]) * size)
                ps.append(flip(me, name))
                base = ks[-1]
            keep.append(ks)
            give.append(gs)
            peers.append(ps)
        size_of = [DEVS >> (k + 1) for k in range(STAGES)]

        def rs_copy(k, c, order):
            slot = lax.rem(c, SLOTS[k])
            return pltpu.make_async_remote_copy(
                w_s.at[lax.rem(c, WSLOTS), order, pl.ds(give[order][k], size_of[k])], recv[k].at[slot, order],
                ws.at[k, slot, order], wr.at[k, slot, order],
                device_id=(peers[order][k],), device_id_type=MESH)

        def advance(k, c):
            slot, wslot = lax.rem(c, SLOTS[k]), lax.rem(c, WSLOTS)
            for order in range(2):
                rs_copy(k, c, order).wait()
                mine = pl.ds(keep[order][k], size_of[k])
                total = w_s[wslot, order, mine] + recv[k][slot, order]
                if k < STAGES - 1:
                    w_s[wslot, order, mine] = total
                    rs_copy(k + 1, c, order).start()
                else:
                    d_s[pl.ds(pl.multiple_of(c * ROWS, ROWS), ROWS), order * HALF:(order + 1) * HALF] = total[0]

        def norm_units(c):
            xslot, hslot = lax.rem(c, XSLOTS), lax.rem(c, HSLOTS)

            def unit_of(b):
                def run():
                    xv = x_s[xslot, b * devs_in:(b + 1) * devs_in].reshape(rows_in, dim).astype(F32)
                    inv = lax.rsqrt(jnp.mean(xv * xv, axis=-1, keepdims=True) + NORM_EPS)
                    h_s[hslot, b * rows_in:(b + 1) * rows_in, :] = (xv * inv * g_ref[...]).astype(BF16)
                return run
            return [unit_of(b) for b in range(blocks)]

        def logit_units(c):
            hslot, zslot = lax.rem(c, HSLOTS), lax.rem(c, ZSLOTS)

            def unit_of(lo, width):
                def run():
                    z = lax.dot_general(h_s[hslot], e_s[lo:lo + width, :], (((1,), (1,)), ((), ())), preferred_element_type=F32)
                    z = z * (1.0 / LOGIT_SCALE)
                    if lo + width > first_pad:
                        z = z + bias_s[0:1, lo:lo + width]
                    z_s[zslot, :, lo:lo + width] = z
                return run
            return [unit_of(lo, width) for lo, width in tiles]

        def sum_units(c, out):
            zslot = lax.rem(c, ZSLOTS)

            def unit_of(b):
                def run():
                    rows = slice(b * rows_in, (b + 1) * rows_in)
                    top = z_s[zslot, rows, 0:128]
                    for lo in range(128, vocab_pad, 128):
                        top = jnp.maximum(top, z_s[zslot, rows, lo:lo + 128])
                    m = jnp.max(top, axis=-1, keepdims=True)
                    acc = jnp.exp(z_s[zslot, rows, 0:128] - m)
                    for lo in range(128, vocab_pad, 128):
                        acc = acc + jnp.exp(z_s[zslot, rows, lo:lo + 128] - m)
                    s = jnp.sum(acc, axis=-1, keepdims=True)
                    lane = lax.broadcasted_iota(jnp.int32, (rows_in, 128), 1)
                    out.append(jnp.where(lane == 0, m, s))
                return run
            return [unit_of(b) for b in range(blocks)]

        def send_stats(c, parts):
            slot = lax.rem(c, 4)
            per = 128 // rows_in
            for i in range(4):
                pair = jnp.concatenate(parts[i * per:(i + 1) * per], axis=0).T
                st1[slot, 0, i:i + 1, :] = pair[0:1, :]
                st1[slot, 0, 4 + i:5 + i, :] = pair[1:2, :]
            for r in range(1, 8):
                stat1_copy(c, r).start()

        def merge(ref, slot, n):
            ms = [ref[slot, r, 0:4, :] for r in range(n)]
            ss = [ref[slot, r, 4:8, :] for r in range(n)]
            m = ms[0]
            for v in ms[1:]:
                m = jnp.maximum(m, v)
            s = ss[0] * jnp.exp(ms[0] - m)
            for a, b in zip(ms[1:], ss[1:]):
                s = s + b * jnp.exp(a - m)
            return m, s

        def stats1(c):
            for r in range(1, 8):
                stat1_copy(c, r).wait()
            m, s = merge(st1, lax.rem(c, 4), 8)
            slot = lax.rem(c, 4)
            st2[slot, 0, 0:4, :] = m
            st2[slot, 0, 4:8, :] = s
            for r in range(1, 4):
                stat2_copy(c, r).start()

        def token_columns(c):
            for r in range(1, 4):
                stat2_copy(c, r).wait()
            m, s = merge(st2, lax.rem(c, 4), 4)
            lse = m + jnp.log(s)
            code = tbl_ref[pl.ds(c, 1), :] * 0.5
            label = jnp.floor(code)
            local = label - first_id
            p_s[0:1, :] = jnp.where(local < float(vocab), local, -1.0)
            p_s[1:2, :] = 2.0 * (code - label) * unit
            for i in range(4):
                p_s[2:3, i * 128:(i + 1) * 128] = lse[i:i + 1, :]
            return p_s[...].T

        def dz_units(c, cols):
            zslot = lax.rem(c, ZSLOTS)

            def unit_of(b):
                def run():
                    rows = slice(b * rows_in, (b + 1) * rows_in)
                    label, weight, lse = (cols[rows, k:k + 1] for k in range(3))
                    hit_sum = jnp.zeros((rows_in, 128), F32)
                    for lo, width in tiles:
                        z = z_s[zslot, rows, lo:lo + width]
                        p = jnp.exp(z - lse)
                        col = lax.broadcasted_iota(jnp.int32, (1, width), 1).astype(F32) + float(lo)
                        hit = col == label
                        dz_s[rows, lo:lo + width] = (jnp.where(hit, p - 1.0, p) * weight).astype(BF16)
                        hz = jnp.where(hit, z, 0.0)
                        for i in range(0, width, 128):
                            hit_sum = hit_sum + hz[:, i:i + 128]
                    row = lax.broadcasted_iota(jnp.int32, (rows_in, 1), 0) + b * rows_in
                    own = (row >= me * ROWS) & (row < me * ROWS + ROWS)
                    term = weight * (jnp.where(own, lse, 0.0) - jnp.sum(hit_sum, axis=-1, keepdims=True))
                    loss_s[...] += jnp.sum(term, axis=0, keepdims=True)
                return run
            return [unit_of(b) for b in range(blocks)]

        def dh_units(c):
            wslot = lax.rem(c, WSLOTS)

            def unit_of(n):
                def run():
                    order, lo = divmod(n * 256, HALF)
                    dh = jnp.dot(dz_s[...], e_s[:, n * 256:(n + 1) * 256], preferred_element_type=F32)
                    for dev in range(DEVS):
                        w_s[wslot, order, block_of(order, dev), :, lo:lo + 256] = dh[dev * ROWS:(dev + 1) * ROWS, :]
                return run
            return [unit_of(n) for n in range(dim // 256)]

        def table_units(c):
            hslot = lax.rem(c, HSLOTS)

            def unit_of(lo, width):
                def run():
                    de_s[lo:lo + width, :] += lax.dot_general(
                        dz_s[:, lo:lo + width], h_s[hslot], (((0,), (0,)), ((), ())), preferred_element_type=F32)
                return run
            return [unit_of(lo, width) for lo, width in row_tiles]

        def last_gain(c):
            xslot, wslot = lax.rem(c, XSLOTS), lax.rem(c, WSLOTS)
            gains = [jnp.zeros((ROWS, HALF), F32) for _ in range(2)]
            for dev in range(DEVS):
                xv = x_s[xslot, dev].astype(F32)
                xh = xv * lax.rsqrt(jnp.mean(xv * xv, axis=-1, keepdims=True) + NORM_EPS)
                for order in range(2):
                    gains[order] = gains[order] + xh[:, order * HALF:(order + 1) * HALF] * w_s[wslot, order, block_of(order, dev)]
            for order in range(2):
                late_s[0:1, order * HALF:(order + 1) * HALF] = jnp.sum(gains[order], axis=0, keepdims=True) * (1.0 / LOGIT_SCALE)

        def block_a(i, norm, table):
            for run in (table_units(i - LAG - 1) if table else []) + (norm_units(i + 1) if norm else []):
                run()

        def block_b(i, fwd, bwd):
            cols = token_columns(i - LAG) if bwd else None
            parts = []
            unit_lists = {"L": logit_units(i) if fwd else [], "Z": dz_units(i - LAG, cols) if bwd else [],
                          "D": dh_units(i - LAG) if bwd else [], "S": sum_units(i, parts) if fwd else []}
            for name in "LZDS":
                for run in unit_lists[name]:
                    run()
            if bwd:
                for order in range(2):
                    rs_copy(0, i - LAG, order).start()
            if fwd:
                send_stats(i, parts)

        def either(low, high, i, first, run):
            a, b = i < first, (i >= low) & (i < high)
            pl.when(a & b)(lambda: run(i, True, True))
            pl.when(a & jnp.logical_not(b))(lambda: run(i, True, False))
            pl.when(jnp.logical_not(a) & b)(lambda: run(i, False, True))

        zid, pid = me // 8, lax.rem(me, 8)

        def own_rows(lo, n):
            xv = xo_s[lo // ROWS:(lo + n) // ROWS].reshape(n, dim).astype(F32)
            inv = lax.rsqrt(jnp.mean(xv * xv, axis=-1, keepdims=True) + NORM_EPS)
            xh = xv * inv
            dh = d_s[lo:lo + n, :] * (1.0 / LOGIT_SCALE)
            u = dh * g_ref[...]
            dxo_s[lo:lo + n, :] = inv * (u - xh * jnp.mean(u * xh, axis=-1, keepdims=True))
            return dh * xh

        def fin_copy(buf, at, r, ss, rs, dev):
            return pltpu.make_async_remote_copy(
                buf.at[at], buf.at[at], ss.at[r], rs.at[r], device_id=(dev,), device_id_type=MESH)

        first = [fin_copy(fin1, pid, r, f1s, f1r, plane_peer(r)) for r in range(1, 8)]
        second = [fin_copy(fin2, zid, r, f2s, f2r, z_peer(r)) for r in range(1, 4)]

        def early_rows():
            gain = jnp.sum(own_rows(0, (chunks - 1) * ROWS), axis=0, keepdims=True) + late_s[0:1, :]
            for i in range(8):
                fin1[pid, i:i + 1, :] = gain[:, i * 128:(i + 1) * 128]
            fin1[pid, 8:16, :] = jnp.broadcast_to(loss_s[0:1, :], (8, 128))
            for c in first:
                c.start()

        def merge_plane():
            for c in first:
                c.wait()
            total = fin1[0]
            for i in range(1, 8):
                total = total + fin1[i]
            fin2[zid] = total
            for c in second:
                c.start()

        x_copy(0).wait()
        for run in norm_units(0):
            run()
        de_s[...] = jnp.zeros_like(de_s)
        e_copy.wait()
        rows = lax.broadcasted_iota(jnp.int32, (vocab_pad - first_pad, 1), 0) + first_pad
        tail = e_s[pl.ds(first_pad, vocab_pad - first_pad), :]
        e_s[pl.ds(first_pad, vocab_pad - first_pad), :] = jnp.where(
            rows + me * vocab < VOCAB_REAL, tail, jnp.zeros_like(tail))
        xo_copy.wait()
        pl.semaphore_wait(barrier, 10)

        de_copy = pltpu.make_async_copy(de_s, de_ref, o_sem.at[0])

        def step(i, carry):
            @pl.when((i >= 0) & (i + 2 < chunks))
            def _():
                x_copy(i + 2).start()

            @pl.when(i + 1 < chunks)
            def _():
                x_copy(i + 1).wait()

            either(LAG + 1, chunks + LAG + 1, i, chunks - 1, block_a)

            @pl.when(i == chunks + LAG)
            def _():
                de_s[...] = de_s[...] * (1.0 / LOGIT_SCALE)

            @pl.when(i == chunks + LAG + 1)
            def _():
                de_copy.start()

            for k in reversed(range(STAGES)):
                @pl.when((i >= WAIT_AT[k]) & (i < chunks + WAIT_AT[k]))
                def _(k=k):
                    advance(k, i - WAIT_AT[k])

            either(LAG, chunks + LAG, i, chunks, block_b)

            @pl.when((i >= 1) & (i < chunks + 1))
            def _():
                stats1(i - 1)

            @pl.when(i == chunks + LAG - 1)
            def _():
                last_gain(chunks - 1)

            @pl.when(i == chunks - 2 + WAIT_AT[-1])
            def _():
                early_rows()

            return carry

        lax.fori_loop(0, chunks - 1 + WAIT_AT[-1], step, 0)

        last = chunks - 1
        merge_plane()
        advance(STAGES - 1, last)
        own_rows(last * ROWS, ROWS)
        dx_copy = pltpu.make_async_copy(dxo_s, dx_ref, o_sem.at[1])
        dx_copy.start()
        for c in second:
            c.wait()
        total = fin2[0]
        for i in range(1, 4):
            total = total + fin2[i]
        fin_ref[...] = total
        dx_copy.wait()
        de_copy.wait()

    return kernel


def relay(dx_in, de_in, fin_in, dx_out, de_out, dg_out, loss_out, dx_s, de_s, in_sem, out_sem):
    rows = de_in.shape[0]
    step = rows // 4 // 8 * 8
    spans = [(n * step, step if n < 3 else rows - 3 * step) for n in range(4)]
    reads = [pltpu.make_async_copy(de_in.at[pl.ds(lo, n)], de_s.at[pl.ds(lo, n)], in_sem.at[k]) for k, (lo, n) in enumerate(spans)]
    writes = [pltpu.make_async_copy(de_s.at[pl.ds(lo, n)], de_out.at[pl.ds(lo, n)], out_sem.at[k]) for k, (lo, n) in enumerate(spans)]
    reads.append(pltpu.make_async_copy(dx_in, dx_s, in_sem.at[4]))
    writes.append(pltpu.make_async_copy(dx_s, dx_out, out_sem.at[4]))
    for copy in reads:
        copy.start()
    dg_out[...] = fin_in[0:8, :]
    loss_out[...] = fin_in[8:9, 0:1]
    for read, write in zip(reads, writes):
        read.wait()
        write.start()
    for copy in writes:
        copy.wait()


def solution(mesh):
    def local_step(residual, labels, loss_mask, norm_gain, table_shard):
        tokens, dim = residual.shape
        vocab = table_shard.shape[0]
        vocab_pad = -(-vocab // 128) * 128
        chunks = tokens // CHUNK
        def by_chunk(v):
            return v.reshape(DEVS, chunks, ROWS).transpose(1, 0, 2).reshape(chunks, CHUNK)

        tbl = by_chunk((2 * labels + loss_mask.astype(jnp.int32)).astype(F32))
        anyspec = pl.BlockSpec(memory_space=pl.ANY)
        vspec = pl.BlockSpec(memory_space=pltpu.VMEM)
        sems = pltpu.SemaphoreType.DMA
        dx, de, fin = pl.pallas_call(
            make_kernel(chunks, vocab, vocab_pad, dim),
            out_shape=(jax.ShapeDtypeStruct((chunks * ROWS, dim), F32),
                       jax.ShapeDtypeStruct((vocab, dim), F32),
                       jax.ShapeDtypeStruct((16, 128), F32)),
            in_specs=[anyspec, anyspec, vspec, vspec],
            out_specs=(anyspec, anyspec, vspec),
            scratch_shapes=[
                pltpu.VMEM((vocab, dim), F32),
                pltpu.VMEM((8, vocab_pad), F32),
                pltpu.VMEM((vocab_pad, dim), BF16),
                pltpu.VMEM((XSLOTS, DEVS, ROWS, dim), BF16),
                pltpu.VMEM((HSLOTS, CHUNK, dim), BF16),
                pltpu.VMEM((ZSLOTS, CHUNK, vocab_pad), F32),
                pltpu.VMEM((CHUNK, vocab_pad), BF16),
                pltpu.VMEM((WSLOTS, 2, DEVS, ROWS, HALF), F32),
                *[pltpu.VMEM((SLOTS[k], 2, DEVS >> (k + 1), ROWS, HALF), F32) for k in range(STAGES)],
                pltpu.VMEM((chunks * ROWS, dim), F32),
                pltpu.VMEM((4, 8, 8, 128), F32),
                pltpu.VMEM((4, 4, 8, 128), F32),
                pltpu.VMEM((8, CHUNK), F32),
                pltpu.VMEM((8, 128), F32),
                pltpu.VMEM((chunks, ROWS, dim), BF16),
                pltpu.VMEM((8, 16, 128), F32),
                pltpu.VMEM((4, 16, 128), F32),
                pltpu.VMEM((chunks * ROWS, dim), F32),
                pltpu.VMEM((8, dim), F32),
                sems((2,)), sems((2,)),
                sems((4, 8)), sems((4, 8)), sems((4, 4)), sems((4, 4)),
                sems((STAGES, 4, 2)), sems((STAGES, 4, 2)),
                sems((8,)), sems((8,)), sems((4,)), sems((4,)), sems((2,)),
            ],
            compiler_params=pltpu.CompilerParams(collective_id=0, has_side_effects=True, vmem_limit_bytes=62 * 1024 * 1024),
        )(residual.reshape(DEVS, chunks, ROWS, dim), table_shard, norm_gain.reshape(1, dim), tbl)
        dx, de, dg, loss = pl.pallas_call(
            relay,
            out_shape=(jax.ShapeDtypeStruct(dx.shape, F32), jax.ShapeDtypeStruct(de.shape, F32),
                       jax.ShapeDtypeStruct((8, 128), F32), jax.ShapeDtypeStruct((1, 1), F32)),
            in_specs=[anyspec, anyspec, vspec],
            out_specs=(anyspec, anyspec, vspec, vspec),
            scratch_shapes=[pltpu.VMEM(dx.shape, F32), pltpu.VMEM(de.shape, F32), sems((5,)), sems((5,))],
        )(dx, de, fin)
        return loss[0, 0], dx, de, dg.reshape(dim)

    return jax.shard_map(
        local_step, mesh=mesh, in_specs=(P(), P(), P(), P(), P("vp", None)),
        out_specs=(P(), P("vp", None), P("vp", None), P()), check_vma=False)
```
